32 devices in a mesh: group: 2 (over y), cp: 8 (over z, x), hd: 2 (over core).
Axes of the slice: x: 2, y: 2, z: 4, core: 2. Of those that a mesh axis runs over, the one named last changes fastest.
Arguments:
- doc_lengths: int32 [8], P('group'), parts along dimension 0, may hold values from 1 to 384, 1024 in all
- queries: bfloat16 [2048, 4096], P(('group', 'cp'), 'hd'), parts along dimension 0, may hold values from -52 to 52
- key_states: bfloat16 [2048, 1024], P(('group', 'cp'), 'hd'), parts along dimension 0, may hold values from -4 to 4
- value_head_states: bfloat16 [2048, 1024], P(('group', 'cp'), 'hd'), parts along dimension 0, may hold values from -6 to 6
- out_grad: bfloat16 [2048, 4096], P(('group', 'cp'), 'hd'), parts along dimension 0, may hold values from -6 to 6
Outputs:
- attended: bfloat16 [2048, 4096], P(('group', 'cp'), 'hd'), parts along dimension 0
- grad_queries: bfloat16 [2048, 4096], P(('group', 'cp'), 'hd'), parts along dimension 0
- grad_keys: bfloat16 [2048, 1024], P(('group', 'cp'), 'hd'), parts along dimension 0
- grad_values: bfloat16 [2048, 1024], P(('group', 'cp'), 'hd'), parts along dimension 0
The draws below stay inside these ranges and needn't reach their ends.
There are 2 independent parts, one for each index of `group`. The reference program is written for one: setup_inputs(seed, part) draws one part's arguments, and reference() takes and returns one part's arrays. A program takes and returns all parts, laid end to end along the dimension named above; each array names one. Nothing has to cross between parts.
Inputs may be any that keep to these rules, and one draw needn't show every extreme that they name: `doc_lengths`: documents lie end to end in token order; their lengths sum to 1024.
All inputs are finite; a program needn't handle non-finite values.
Results may differ from the reference program's by a relative error of at most 0.028.
Values may be sent and summed in bfloat16 or wider, within the bound.
No kernel may reach another device: no remote copies, remote signals or barrier semaphores. Data moves between devices by JAX's collectives and lax.ppermute only.
A program may use at most 64 MiB of HBM per device.

```python
import math
import jax
import jax.numpy as jnp
import numpy as np
from jax import lax

QUERY_HEADS_COUNT = 32
KEY_VALUE_HEADS = 8
HEAD_SIZE = 128
TOK_DEV = 128
REACH = 3
WINDOW_TOKENS = 1024
MAXDOC = 384
DOCS = 4
N_CP = 8


def starting_keys(key):
    array_extent = (WINDOW_TOKENS, KEY_VALUE_HEADS * HEAD_SIZE)
    sampled_values = jax.random.truncated_normal(jax.random.fold_in(key, 12), -4.0, 4.0, array_extent, jnp.float32)
    return sampled_values


def draw_key_states(key, part):
    sampled_values = starting_keys(key)
    return sampled_values.astype(jnp.bfloat16)


def draw_queries(key, part):
    array_extent = (WINDOW_TOKENS, QUERY_HEADS_COUNT * HEAD_SIZE)
    sampled_values = jax.random.truncated_normal(jax.random.fold_in(key, 13), -4.0, 4.0, array_extent, jnp.float32)
    return sampled_values.astype(jnp.bfloat16)


def level_of(stream_key, shape, pieces, smallest, high):
    factor_of, own = 1.0, jax.random.fold_in(stream_key, 6)
    for dim, shards_of in pieces:
        draws = jnp.exp(jax.random.uniform(jax.random.fold_in(own, dim), (shards_of,), jnp.float32, smallest / len(pieces), high / len(pieces)))
        factor_of = factor_of * jnp.repeat(draws, shape[dim] // shards_of).reshape([-1 if axis == dim else 1 for axis in range(len(shape))])
    return factor_of


def length_profile(count, total, bound, slope):
    loads = [(1 << 20) // math.isqrt(grade ** slope) + 1 for grade in range(2, count + 1)]
    rest, given = total - bound - (count - 1), [1] * (count - 1)
    while rest > 0:
        candidates = [i for i in range(count - 1) if given[i] < bound]
        pool, budget = sum([loads[i] for i in candidates]), rest
        for i in candidates:
            extra = min(bound - given[i], max(1, budget * loads[i] // pool), rest)
            given[i] = given[i] + extra
            rest = rest - extra
    return np.array([bound] + given)


def uneven_parts(own_key, amount, total, limit, skew):
    if amount == 2:
        one = jax.random.randint(own_key, (), max(1, total - limit), min(limit, total - 1) + 1)
        return jnp.stack([one, total - one])
    lengths = jnp.asarray(length_profile(amount, total, limit, skew), jnp.int32)
    twos = (amount - 1) // 2
    giver, receiver = lengths[1:1 + 2 * twos:2], lengths[2:2 + 2 * twos:2]
    margin = jnp.minimum(giver - 1, limit - receiver)
    passed = jax.random.randint(jax.random.fold_in(own_key, 1), (twos,), 0, 1 << 20) % (margin + 1)
    lengths = lengths.at[1:1 + 2 * twos:2].set(giver - passed).at[2:2 + 2 * twos:2].set(receiver + passed)
    return lengths[jax.random.permutation(jax.random.fold_in(own_key, 2), amount)]


def scatter_about(rng, dims, scale, bound, pieces=(), kind=jnp.bfloat16):
    values = jax.random.normal(rng, dims, jnp.float32) * scale
    if len(pieces) > 0:
        values = level_of(rng, dims, pieces, -0.22, 0.18) * values
    return jnp.clip(values, min=-bound, max=bound).astype(kind)


def setup_inputs(seed: int = 0, part: int = 0) -> dict:
    arg_keys = jax.random.split(jax.random.key(seed), 6)
    own_keys = jax.random.split(jax.random.fold_in(arg_keys[5], part), 6)
    return {
        "doc_lengths": uneven_parts(own_keys[0], DOCS, WINDOW_TOKENS, MAXDOC, 2).astype(jnp.int32),
        "queries": draw_queries(jax.random.fold_in(jax.random.fold_in(arg_keys[5], part), 71), part),
        "key_states": draw_key_states(jax.random.fold_in(jax.random.fold_in(arg_keys[5], part), 71), part),
        "value_head_states": scatter_about(own_keys[3], (WINDOW_TOKENS, KEY_VALUE_HEADS * HEAD_SIZE), 1.0, 6.0, ((0, 8), (1, 2))),
        "out_grad": scatter_about(own_keys[4], (WINDOW_TOKENS, QUERY_HEADS_COUNT * HEAD_SIZE), 1.0, 6.0, ((0, 8), (1, 2))),
    }


masked_score = -1e+30

def document_ids(doc_lengths, positions):
    ends = jnp.cumsum(doc_lengths).astype(jnp.int32)
    counted = lax.optimization_barrier(jnp.sum((ends[None, :] <= positions[:, None]).astype(jnp.int32), axis=1)).astype(jnp.int32)
    return jnp.where(positions < 0, jnp.int32(-1), counted)

def attend(queries, key_rows, value_rows, out_grad, allowed):
    tok_rows = queries.shape[0]
    window_rows = key_rows.shape[0]
    head_kv = key_rows.shape[1] // HEAD_SIZE
    group_size = queries.shape[1] // key_rows.shape[1]
    score_scale = 1.0 / math.sqrt(HEAD_SIZE)
    query_heads = queries.reshape(tok_rows, head_kv, group_size, HEAD_SIZE).astype(jnp.float32)
    key_heads = key_rows.reshape(window_rows, head_kv, HEAD_SIZE).astype(jnp.float32)
    value_heads = value_rows.reshape(window_rows, head_kv, HEAD_SIZE).astype(jnp.float32)
    grad_heads = out_grad.reshape(tok_rows, head_kv, group_size, HEAD_SIZE).astype(jnp.float32)
    scores = jnp.einsum('qhgd,khd->hgqk', query_heads, key_heads) * score_scale
    scores = jnp.where(allowed, scores, masked_score)
    row_max = lax.optimization_barrier(jnp.max(scores, axis=-1, keepdims=True))
    weights_raw = jnp.exp(scores - row_max)
    probs = weights_raw / lax.optimization_barrier(jnp.sum(weights_raw, axis=-1, keepdims=True))
    probs_low = probs.astype(jnp.bfloat16).astype(jnp.float32)
    attended = jnp.einsum('hgqk,khd->qhgd', probs_low, value_heads).astype(jnp.bfloat16)
    delta = lax.optimization_barrier(jnp.sum(grad_heads * attended.astype(jnp.float32), axis=-1)).transpose(1, 2, 0)
    grad_value = jnp.einsum('hgqk,qhgd->khd', probs_low, grad_heads)
    grad_probs = jnp.einsum('qhgd,khd->hgqk', grad_heads, value_heads)
    grad_scores = (probs * (grad_probs - delta[..., None])).astype(jnp.bfloat16).astype(jnp.float32)
    grad_query = (jnp.einsum('hgqk,khd->qhgd', grad_scores, key_heads) * score_scale).astype(jnp.bfloat16)
    grad_key = jnp.einsum('hgqk,qhgd->khd', grad_scores, query_heads) * score_scale
    return (attended.reshape(tok_rows, -1), grad_query.reshape(tok_rows, -1), grad_key.reshape(window_rows, -1), grad_value.reshape(window_rows, -1))

def reference(doc_lengths, queries, key_states, value_head_states, out_grad):
    tok_rows = TOK_DEV
    window_rows = (REACH + 1) * tok_rows
    pad_rows = REACH * tok_rows
    columns = key_states.shape[1]
    padding = jnp.zeros((pad_rows, columns), key_states.dtype)
    keys_padded = jnp.concatenate([padding, key_states], axis=0)
    values_padded = jnp.concatenate([padding, value_head_states], axis=0)
    empty = jnp.zeros((pad_rows + WINDOW_TOKENS, columns), jnp.float32)

    def block_step(carry, block_index):
        sum_keys, sum_values = carry
        row_start = (block_index * tok_rows).astype(jnp.int32)
        query_block = lax.dynamic_slice_in_dim(queries, row_start, tok_rows, 0)
        grad_block = lax.dynamic_slice_in_dim(out_grad, row_start, tok_rows, 0)
        key_block = lax.dynamic_slice_in_dim(keys_padded, row_start, window_rows, 0)
        value_block = lax.dynamic_slice_in_dim(values_padded, row_start, window_rows, 0)
        query_pos = row_start + lax.iota(jnp.int32, tok_rows)
        key_pos = row_start - pad_rows + lax.iota(jnp.int32, window_rows)
        query_ids = document_ids(doc_lengths, query_pos)
        key_ids = document_ids(doc_lengths, key_pos)
        allowed = (query_ids[:, None] == key_ids[None, :]) & (key_pos[None, :] <= query_pos[:, None])
        attended, grad_query, grad_key, grad_value = attend(query_block, key_block, value_block, grad_block, allowed)
        old_keys = lax.dynamic_slice_in_dim(sum_keys, row_start, window_rows, 0)
        old_values = lax.dynamic_slice_in_dim(sum_values, row_start, window_rows, 0)
        sum_keys = lax.dynamic_update_slice_in_dim(sum_keys, old_keys + grad_key, row_start, 0)
        sum_values = lax.dynamic_update_slice_in_dim(sum_values, old_values + grad_value, row_start, 0)
        return ((sum_keys, sum_values), (attended, grad_query))
    (sum_keys, sum_values), (outs, grads) = lax.scan(block_step, (empty, empty), jnp.arange(N_CP, dtype=jnp.int32))
    attended = outs.reshape(WINDOW_TOKENS, -1)
    grad_queries = grads.reshape(WINDOW_TOKENS, -1)
    grad_keys = sum_keys[pad_rows:].astype(jnp.bfloat16)
    grad_values = sum_values[pad_rows:].astype(jnp.bfloat16)
    return (attended, grad_queries, grad_keys, grad_values)
```

```python
import functools
import math

import jax
import jax.numpy as jnp
from jax import lax
from jax.experimental import pallas as pl
from jax.experimental.pallas import tpu as pltpu
from jax.sharding import PartitionSpec as P

HEAD = 128
MASKED = -1e30


def shift(value, by):
    peers = lax.axis_size("cp")
    pairs = [(i, i + by) for i in range(peers) if 0 <= i + by < peers]
    return lax.ppermute(value, "cp", pairs)


def dot(a, b, contract):
    return lax.dot_general(a, b, (contract, ((), ())), preferred_element_type=jnp.float32)


def stacked(block):
    heads = block.shape[1] // HEAD
    return jnp.concatenate([block[:, i * HEAD:(i + 1) * HEAD] for i in range(heads)], axis=0)


def attention_kernel(tok, lens_ref, pos_ref, q_ref, do_ref, k_ref, v_ref, near_ref, mid_ref,
                     o_ref, dq_ref, own_ref, gmid_ref, gnear_ref):
    heads = q_ref.shape[1] // HEAD
    scale = 1.0 / math.sqrt(HEAD)
    start = pos_ref[0]
    query_pos = start + lax.broadcasted_iota(jnp.int32, (1, tok), 1)

    def place(d, carry):
        end, low = carry
        end = end + lens_ref[d]
        return end, jnp.where(end <= query_pos, end, low)

    _, low = lax.fori_loop(0, lens_ref.shape[0], place, (jnp.int32(0), jnp.zeros((1, tok), jnp.int32)))
    low = jnp.concatenate([low - start] * heads, axis=1)
    rel = lax.broadcasted_iota(jnp.int32, (4 * tok, tok * heads), 0) - 3 * tok
    upto = jnp.concatenate([query_pos - start] * heads, axis=1)
    allowed = (rel >= low) & (rel <= upto)

    keys = jnp.concatenate([near_ref[2 * tok:3 * tok], mid_ref[:tok], near_ref[:tok], k_ref[...]], axis=0)
    values = jnp.concatenate([near_ref[3 * tok:], mid_ref[tok:], near_ref[tok:2 * tok], v_ref[...]], axis=0)
    q = stacked(q_ref[...])
    do = stacked(do_ref[...])
    s = dot(keys, q, ((1,), (1,))) * scale
    s = jnp.where(allowed, s, MASKED)
    e = jnp.exp(s - jnp.max(s, axis=0, keepdims=True))
    p = e * (1.0 / jnp.sum(e, axis=0, keepdims=True))
    p_low = p.astype(jnp.bfloat16)
    dp = dot(values, do, ((1,), (1,)))
    delta = jnp.sum(p * dp, axis=0, keepdims=True)
    ds = (p * (dp - delta)).astype(jnp.bfloat16)
    dv = dot(p_low, do, ((1,), (0,)))
    dk = dot(ds, q, ((1,), (0,))) * scale
    gnear_ref[:tok] = dk[2 * tok:3 * tok].astype(gnear_ref.dtype)
    gnear_ref[tok:2 * tok] = dv[2 * tok:3 * tok].astype(gnear_ref.dtype)
    gnear_ref[2 * tok:3 * tok] = dk[:tok].astype(gnear_ref.dtype)
    gnear_ref[3 * tok:] = dv[:tok].astype(gnear_ref.dtype)
    gmid_ref[:tok] = dk[tok:2 * tok]
    gmid_ref[tok:] = dv[tok:2 * tok]
    own_ref[:tok] = dk[3 * tok:]
    own_ref[tok:] = dv[3 * tok:]
    ot = dot(values, p_low, ((0,), (0,)))
    dqt = dot(keys, ds, ((0,), (0,))) * scale
    for i in range(heads):
        o_ref[:, i * HEAD:(i + 1) * HEAD] = ot[:, i * tok:(i + 1) * tok].T.astype(o_ref.dtype)
        dq_ref[:, i * HEAD:(i + 1) * HEAD] = dqt[:, i * tok:(i + 1) * tok].T.astype(dq_ref.dtype)


def attend(doc_lengths, start, queries, out_grad, keys, values, near, mid):
    tok, width = queries.shape
    kv_width = keys.shape[1]
    kv_heads = kv_width // HEAD
    wide = width // kv_heads

    def col(rows, cols):
        return pl.BlockSpec((rows, cols), lambda h: (0, h))

    smem = pl.BlockSpec(memory_space=pltpu.SMEM)
    f32, low = jnp.float32, queries.dtype
    return pl.pallas_call(
        functools.partial(attention_kernel, tok),
        grid=(kv_heads,),
        in_specs=[smem, smem, col(tok, wide), col(tok, wide), col(tok, HEAD), col(tok, HEAD),
                  col(4 * tok, HEAD), col(2 * tok, HEAD)],
        out_specs=[col(tok, wide), col(tok, wide), col(2 * tok, HEAD), col(2 * tok, HEAD), col(4 * tok, HEAD)],
        out_shape=[
            jax.ShapeDtypeStruct((tok, width), low),
            jax.ShapeDtypeStruct((tok, width), low),
            jax.ShapeDtypeStruct((2 * tok, kv_width), f32),
            jax.ShapeDtypeStruct((2 * tok, kv_width), f32),
            jax.ShapeDtypeStruct((4 * tok, kv_width), low),
        ],
        cost_estimate=pl.CostEstimate(
            flops=40 * tok * tok * width, bytes_accessed=8 * tok * width, transcendentals=4 * tok * tok * kv_heads
        ),
    )(doc_lengths, start, queries, out_grad, keys, values, near, mid)


def shards(doc_lengths, queries, key_states, value_head_states, out_grad):
    tok = queries.shape[0]
    start = (lax.axis_index("cp") * tok).astype(jnp.int32).reshape(1)
    own = jnp.concatenate([key_states, value_head_states], axis=0)
    mid = shift(own, 2)
    near = shift(jnp.concatenate([own, mid], axis=0), 1)
    attended, grad_queries, g_own, g_mid, g_near = attend(
        doc_lengths, start, queries, out_grad, key_states, value_head_states, near, mid
    )
    back = shift(g_near, -1).astype(jnp.float32)
    far = shift((g_mid + back[2 * tok:]).astype(g_near.dtype), -2)
    total = (g_own + back[:2 * tok] + far.astype(jnp.float32)).astype(key_states.dtype)
    return attended, grad_queries, total[:tok], total[tok:]


def solution(mesh):
    part = P(("group", "cp"), "hd")
    return jax.shard_map(
        shards,
        mesh=mesh,
        in_specs=(P("group"), part, part, part, part),
        out_specs=(part, part, part, part),
        check_vma=False,
    )
```

```python
import functools
import math

import jax
import jax.numpy as jnp
from jax import lax
from jax.experimental import pallas as pl
from jax.experimental.pallas import tpu as pltpu
from jax.sharding import PartitionSpec as P

HEAD = 128
MASKED = -1e30


def shift(value, by):
    peers = lax.axis_size("cp")
    return lax.ppermute(value, "cp", [(i, (i + by) % peers) for i in range(peers)])


def dot(a, b, contract):
    return lax.dot_general(a, b, (contract, ((), ())), preferred_element_type=jnp.float32)


def stacked(block):
    heads = block.shape[1] // HEAD
    return jnp.concatenate([block[:, i * HEAD:(i + 1) * HEAD] for i in range(heads)], axis=0)


def attention_kernel(tok, lens_ref, pos_ref, q_ref, do_ref, k_ref, v_ref, near_ref, mid_ref, *rest):
    o_ref, dq_ref, own_ref, gmid_ref, gnear_ref = rest[-5:]
    heads = q_ref.shape[1] // HEAD
    scale = 1.0 / math.sqrt(HEAD)
    start = pos_ref[0]
    query_pos = start + lax.broadcasted_iota(jnp.int32, (1, tok), 1)

    def place(d, carry):
        end, low = carry
        end = end + lens_ref[d]
        return end, jnp.where(end <= query_pos, end, low)

    _, low = lax.fori_loop(0, lens_ref.shape[0], place, (jnp.int32(0), jnp.zeros((1, tok), jnp.int32)))
    low = jnp.concatenate([low - start] * heads, axis=1)
    rel = lax.broadcasted_iota(jnp.int32, (4 * tok, tok * heads), 0) - 3 * tok
    upto = jnp.concatenate([query_pos - start] * heads, axis=1)
    allowed = (rel >= low) & (rel <= upto)

    keys = jnp.concatenate([near_ref[2 * tok:3 * tok], mid_ref[:tok], near_ref[:tok], k_ref[...]], axis=0)
    values = jnp.concatenate([near_ref[3 * tok:], mid_ref[tok:], near_ref[tok:2 * tok], v_ref[...]], axis=0)
    q = stacked(q_ref[...])
    do = stacked(do_ref[...])
    s = dot(keys, q, ((1,), (1,))) * scale
    s = jnp.where(allowed, s, MASKED)
    e = jnp.exp(s - jnp.max(s, axis=0, keepdims=True))
    p = e * (1.0 / jnp.sum(e, axis=0, keepdims=True))
    p_low = p.astype(jnp.bfloat16)
    dp = dot(values, do, ((1,), (1,)))
    delta = jnp.sum(p * dp, axis=0, keepdims=True)
    ds = (p * (dp - delta)).astype(jnp.bfloat16)
    dv = dot(p_low, do, ((1,), (0,)))
    dk = dot(ds, q, ((1,), (0,))) * scale
    gnear_ref[:tok] = dk[2 * tok:3 * tok].astype(gnear_ref.dtype)
    gnear_ref[tok:2 * tok] = dv[2 * tok:3 * tok].astype(gnear_ref.dtype)
    gnear_ref[2 * tok:3 * tok] = dk[:tok].astype(gnear_ref.dtype)
    gnear_ref[3 * tok:] = dv[:tok].astype(gnear_ref.dtype)
    gmid_ref[:tok] = dk[tok:2 * tok]
    gmid_ref[tok:] = dv[tok:2 * tok]
    own_ref[:tok] = dk[3 * tok:]
    own_ref[tok:] = dv[3 * tok:]
    ot = dot(values, p_low, ((0,), (0,)))
    dqt = dot(keys, ds, ((0,), (0,))) * scale
    for i in range(heads):
        o_ref[:, i * HEAD:(i + 1) * HEAD] = ot[:, i * tok:(i + 1) * tok].T.astype(o_ref.dtype)
        dq_ref[:, i * HEAD:(i + 1) * HEAD] = dqt[:, i * tok:(i + 1) * tok].T.astype(dq_ref.dtype)


def attend(doc_lengths, start, queries, out_grad, keys, values, near, mid, first, done):
    tok, width = queries.shape
    kv_heads = near.shape[1] // HEAD
    wide = width // (keys.shape[1] // HEAD)

    def col(rows, cols, offset=0):
        return pl.BlockSpec((rows, cols), lambda h: (0, h + offset))

    smem = pl.BlockSpec(memory_space=pltpu.SMEM)
    f32, low = jnp.float32, queries.dtype
    kv_width = kv_heads * HEAD
    return pl.pallas_call(
        functools.partial(attention_kernel, tok),
        grid=(kv_heads,),
        in_specs=[smem, smem, col(tok, wide, first), col(tok, wide, first), col(tok, HEAD, first),
                  col(tok, HEAD, first), col(4 * tok, HEAD), col(2 * tok, HEAD)]
        + [pl.BlockSpec(memory_space=pl.ANY)] * len(done),
        out_specs=[col(tok, wide, first), col(tok, wide, first), col(2 * tok, HEAD), col(2 * tok, HEAD),
                   col(4 * tok, HEAD)],
        out_shape=[
            jax.ShapeDtypeStruct((tok, width), low),
            jax.ShapeDtypeStruct((tok, width), low),
            jax.ShapeDtypeStruct((2 * tok, kv_width), f32),
            jax.ShapeDtypeStruct((2 * tok, kv_width), f32),
            jax.ShapeDtypeStruct((4 * tok, kv_width), low),
        ],
        input_output_aliases={8 + i: i for i in range(len(done))},
        compiler_params=pltpu.CompilerParams(vmem_limit_bytes=24 * 1024 * 1024),
        cost_estimate=pl.CostEstimate(
            flops=160 * tok * tok * wide * kv_heads, bytes_accessed=8 * tok * width, transcendentals=0
        ),
    )(doc_lengths, start, queries, out_grad, keys, values, near, mid, *done)


def shards(doc_lengths, queries, key_states, value_head_states, out_grad):
    tok = queries.shape[0]
    start = (lax.axis_index("cp") * tok).astype(jnp.int32).reshape(1)
    firsts = range(key_states.shape[1] // HEAD)
    cols = [slice(f * HEAD, (f + 1) * HEAD) for f in firsts]
    own = [jnp.concatenate([key_states[:, c], value_head_states[:, c]], axis=0) for c in cols]
    mid = [shift(o, 2) for o in own]
    near = [shift(jnp.concatenate([o, m], axis=0), 1) for o, m in zip(own, mid)]
    done = ()
    partial = []
    for i, f in enumerate(firsts):
        *done, g_own, g_mid, g_near = attend(
            doc_lengths, start, queries, out_grad, key_states, value_head_states, near[i], mid[i], f, done
        )
        partial.append((g_own, g_mid, g_near))
    total = []
    backs = [shift(g_near, -1).astype(jnp.float32) for _, _, g_near in partial]
    fars = [shift((g_mid + b[2 * tok:]).astype(g_near.dtype), -2) for (_, g_mid, g_near), b in zip(partial, backs)]
    total = [
        (g_own + b[:2 * tok] + far.astype(jnp.float32)).astype(key_states.dtype)
        for (g_own, _, _), b, far in zip(partial, backs, fars)
    ]
    total = jnp.concatenate(total, axis=1)
    return *done, total[:tok], total[tok:]


def solution(mesh):
    part = P(("group", "cp"), "hd")
    return jax.shard_map(
        shards,
        mesh=mesh,
        in_specs=(P("group"), part, part, part, part),
        out_specs=(part, part, part, part),
        check_vma=False,
    )
```

```python
import functools
import math

import jax
import jax.numpy as jnp
from jax import lax
from jax.experimental import pallas as pl
from jax.experimental.pallas import tpu as pltpu
from jax.sharding import PartitionSpec as P

HEAD = 128
MASKED = -1e30
LOG2E = 1.4426950408889634


def shift(value, by):
    peers = lax.axis_size("cp")
    return lax.ppermute(value, "cp", [(i, (i + by) % peers) for i in range(peers)])


def dot(a, b, contract):
    return lax.dot_general(a, b, (contract, ((), ())), preferred_element_type=jnp.float32)


def stacked(block):
    heads = block.shape[1] // HEAD
    return jnp.concatenate([block[:, i * HEAD:(i + 1) * HEAD] for i in range(heads)], axis=0)


def attention_kernel(tok, heads_of, wide, lens_ref, pos_ref, q_ref, do_ref, k_ref, v_ref, *rest):
    count = len(heads_of)
    windows, outs = rest[:2 * count], rest[2 * count:]
    o_ref, dq_ref, own_ref, gmid_ref, gnear_ref = outs
    heads = wide // HEAD
    scale = 1.0 / math.sqrt(HEAD)
    start = pos_ref[0]
    query_pos = start + lax.broadcasted_iota(jnp.int32, (1, tok), 1)

    def place(d, carry):
        end, low = carry
        end = end + lens_ref[d]
        return end, jnp.where(end <= query_pos, end, low)

    _, low = lax.fori_loop(0, lens_ref.shape[0], place, (jnp.int32(0), jnp.zeros((1, tok), jnp.int32)))
    rel = lax.broadcasted_iota(jnp.int32, (4 * tok, tok), 0) - 3 * tok
    bias = jnp.where((rel >= low - start) & (rel <= query_pos - start), 0.0, MASKED)
    bias = jnp.concatenate([bias] * heads, axis=1)
    for c, (head, near_at, mid_at) in enumerate(heads_of):
        near_ref, mid_ref = windows[2 * c:2 * c + 2]
        near_kv = slice(near_at * HEAD, (near_at + 1) * HEAD)
        mid_kv = slice(mid_at * HEAD, (mid_at + 1) * HEAD)
        kv = slice(c * HEAD, (c + 1) * HEAD)
        mine = slice(head * HEAD, (head + 1) * HEAD)
        cols = slice(head * wide, (head + 1) * wide)
        keys = jnp.concatenate(
            [near_ref[2 * tok:3 * tok, near_kv], mid_ref[:tok, mid_kv], near_ref[:tok, near_kv], k_ref[:, mine]], axis=0
        )
        values = jnp.concatenate(
            [near_ref[3 * tok:, near_kv], mid_ref[tok:, mid_kv], near_ref[tok:2 * tok, near_kv], v_ref[:, mine]], axis=0
        )
        q = stacked(q_ref[:, cols])
        do = stacked(do_ref[:, cols])
        s = dot(keys, q, ((1,), (1,))) * (scale * LOG2E) + bias
        dp = dot(values, do, ((1,), (1,)))
        e = jnp.exp2(s - jnp.max(s, axis=0, keepdims=True))
        p = e * (1.0 / jnp.sum(e, axis=0, keepdims=True))
        p_low = p.astype(jnp.bfloat16)
        delta = jnp.sum(p * dp, axis=0, keepdims=True)
        ds = (p * (dp - delta)).astype(jnp.bfloat16)
        ot = dot(values, p_low, ((0,), (0,)))
        dqt = dot(keys, ds, ((0,), (0,))) * scale
        for i in range(heads):
            to = slice(c * wide + i * HEAD, c * wide + (i + 1) * HEAD)
            o_ref[:, to] = ot[:, i * tok:(i + 1) * tok].T.astype(o_ref.dtype)
            dq_ref[:, to] = dqt[:, i * tok:(i + 1) * tok].T.astype(dq_ref.dtype)
        dv = dot(p_low, do, ((1,), (0,)))
        dk = dot(ds, q, ((1,), (0,))) * scale
        gnear_ref[:tok, kv] = dk[2 * tok:3 * tok].astype(gnear_ref.dtype)
        gnear_ref[tok:2 * tok, kv] = dv[2 * tok:3 * tok].astype(gnear_ref.dtype)
        gnear_ref[2 * tok:3 * tok, kv] = dk[:tok].astype(gnear_ref.dtype)
        gnear_ref[3 * tok:, kv] = dv[:tok].astype(gnear_ref.dtype)
        gmid_ref[:tok, kv] = dk[tok:2 * tok]
        gmid_ref[tok:, kv] = dv[tok:2 * tok]
        own_ref[:tok, kv] = dk[3 * tok:]
        own_ref[tok:, kv] = dv[3 * tok:]


def attend(doc_lengths, start, queries, out_grad, keys, values, windows, heads_of):
    tok, width = queries.shape
    wide = width // (keys.shape[1] // HEAD)
    count = len(heads_of)
    smem = pl.BlockSpec(memory_space=pltpu.SMEM)
    vmem = pl.BlockSpec(memory_space=pltpu.VMEM)
    f32, low = jnp.float32, queries.dtype
    return pl.pallas_call(
        functools.partial(attention_kernel, tok, heads_of, wide),
        in_specs=[smem, smem] + [vmem] * (4 + len(windows)),
        out_specs=[vmem] * 5,
        out_shape=[
            jax.ShapeDtypeStruct((tok, wide * count), low),
            jax.ShapeDtypeStruct((tok, wide * count), low),
            jax.ShapeDtypeStruct((2 * tok, HEAD * count), f32),
            jax.ShapeDtypeStruct((2 * tok, HEAD * count), f32),
            jax.ShapeDtypeStruct((4 * tok, HEAD * count), low),
        ],
        compiler_params=pltpu.CompilerParams(vmem_limit_bytes=24 * 1024 * 1024),
        cost_estimate=pl.CostEstimate(
            flops=160 * tok * tok * wide * count, bytes_accessed=8 * tok * width, transcendentals=0
        ),
    )(doc_lengths, start, queries, out_grad, keys, values, *windows)


def cat(parts, axis):
    return parts[0] if len(parts) == 1 else jnp.concatenate(parts, axis=axis)


def part_of(array, at, count=1):
    return array[:, at * HEAD:(at + count) * HEAD]


def shards(doc_lengths, queries, key_states, value_head_states, out_grad):
    tok = queries.shape[0]
    start = (lax.axis_index("cp") * tok).astype(jnp.int32).reshape(1)
    low = key_states.dtype
    count = key_states.shape[1] // HEAD
    single = [(h,) for h in range(count)]
    paired = [tuple(range(count - 2))] + single[count - 2:] if count > 2 else single
    mid, near = {}, {}
    for j, group in enumerate(single):
        with jax.named_scope(f"s1_{j}"):
            own = [part_of(x, group[0], len(group)) for x in (key_states, value_head_states)]
            got = shift(jnp.concatenate(own, axis=0), 2)
        mid.update({h: (got, i) for i, h in enumerate(group)})
    for j, group in enumerate(single):
        with jax.named_scope(f"s2_{j}"):
            own = [part_of(x, group[0], len(group)) for x in (key_states, value_head_states)]
            got = shift(jnp.concatenate(own + [cat([part_of(*mid[h]) for h in group], 1)], axis=0), 1)
        near.update({h: (got, i) for i, h in enumerate(group)})
    outs, dqs, parts = [], [], {}
    for j, group in enumerate(single):
        windows = [x for h in group for x in (near[h][0], mid[h][0])]
        heads_of = [(h, near[h][1], mid[h][1]) for h in group]
        with jax.named_scope(f"k_{j}"):
            o, dq, *grads = attend(
                doc_lengths, start, queries, out_grad, key_states, value_head_states, windows, heads_of
            )
        outs.append(o)
        dqs.append(dq)
        parts.update({h: [part_of(g, i) if len(group) > 1 else g for g in grads] for i, h in enumerate(group)})
    own, onward = {}, {}
    for j, group in enumerate(single):
        with jax.named_scope(f"b1_{j}"):
            back = shift(cat([parts[h][2] for h in group], 1), -1)
        for i, h in enumerate(group):
            got = part_of(back, i).astype(jnp.float32)
            own[h] = parts[h][0] + got[:2 * tok]
            onward[h] = (parts[h][1] + got[2 * tok:]).astype(low)
    total = []
    for j, group in enumerate(paired):
        with jax.named_scope(f"b2_{j}"):
            far = shift(cat([onward[h] for h in group], 1), -2)
        total.append((cat([own[h] for h in group], 1) + far.astype(jnp.float32)).astype(low))
    total = cat(total, 1)
    with jax.named_scope("out_o"):
        attended = cat(outs, 1)
    with jax.named_scope("out_q"):
        grad_queries = cat(dqs, 1)
    return attended, grad_queries, total[:tok], total[tok:]


def solution(mesh):
    part = P(("group", "cp"), "hd")
    return jax.shard_map(
        shards,
        mesh=mesh,
        in_specs=(P("group"), part, part, part, part),
        out_specs=(part, part, part, part),
        check_vma=False,
    )
```
